32 devices in a mesh: dp: 4 (over y, z), tp: 8 (over x, core).
Axes of the slice: x: 4, y: 2, z: 2, core: 2. Of those that a mesh axis runs over, the one named last changes fastest.
The devices are a block of a 4x4x8 slice.
Arguments:
- hidden: bfloat16 [16384, 8192], P(('dp', 'tp')), parts along dimension 0
- norm_gain: float32 [8192], replicated
- w_query: bfloat16 [8192, 64, 128], P(None, 'tp')
- w_key: bfloat16 [8192, 64, 128], P(None, 'tp')
- w_value: bfloat16 [8192, 64, 128], P(None, 'tp')
Outputs:
- output 1: bfloat16 [16384, 64, 128], P('dp', 'tp'), parts along dimension 0
- output 2: bfloat16 [16384, 64, 128], P('dp', 'tp'), parts along dimension 0
- output 3: bfloat16 [16384, 64, 128], P('dp', 'tp'), parts along dimension 0
There are 4 independent parts. The reference program is written for one: setup_inputs(seed, part) draws one part's arguments, and reference() takes and returns one part's arrays. A program takes and returns all parts, laid end to end along the dimension named above; an argument that names none is the same for every part.
All inputs are finite; a program needn't handle non-finite values.
Results may differ from the reference program's by a relative error of at most 0.001.
Values are sent between devices in bfloat16 or wider.
A program may use at most 768 MiB of HBM per device.

```python
import jax
import jax.numpy as jnp
from jax import lax

TOKENS = 4096
MODEL_DIM = 8192
Q_HEADS = 64
KV_COUNT = 64
HEAD_DIM = 128


def setup_inputs(seed: int = 0, part: int = 0) -> dict:
    base_key = jax.random.key(seed)
    part_key = jax.random.fold_in(base_key, part)
    shared = jax.random.split(base_key, 4)
    fan_scale = MODEL_DIM ** -0.5
    hidden = jax.random.normal(part_key, (TOKENS, MODEL_DIM), jnp.float32).astype(jnp.bfloat16)
    norm_gain = jax.random.uniform(shared[0], (MODEL_DIM,), jnp.float32, 0.5, 1.5)
    w_query = (jax.random.normal(shared[1], (MODEL_DIM, Q_HEADS, HEAD_DIM), jnp.float32) * fan_scale).astype(jnp.bfloat16)
    w_key = (jax.random.normal(shared[2], (MODEL_DIM, KV_COUNT, HEAD_DIM), jnp.float32) * fan_scale).astype(jnp.bfloat16)
    w_value = (jax.random.normal(shared[3], (MODEL_DIM, KV_COUNT, HEAD_DIM), jnp.float32) * fan_scale).astype(jnp.bfloat16)
    return {"hidden": hidden, "norm_gain": norm_gain, "w_query": w_query, "w_key": w_key, "w_value": w_value}


def reference(hidden, norm_gain, w_query, w_key, w_value):
    hidden_f32 = hidden.astype(jnp.float32)
    mean_sq = jnp.mean(hidden_f32 * hidden_f32, axis=-1, keepdims=True)
    normed = (hidden_f32 * lax.rsqrt(mean_sq + 1e-6) * norm_gain).astype(jnp.bfloat16)

    def project(weight):
        head_count = weight.shape[1]
        flat_out = jnp.dot(normed, weight.reshape(MODEL_DIM, head_count * HEAD_DIM), preferred_element_type=jnp.float32)
        return flat_out.astype(jnp.bfloat16).reshape(TOKENS, head_count, HEAD_DIM)

    return (project(w_query), project(w_key), project(w_value))
```

```python
import functools

import jax
import jax.numpy as jnp
from jax import lax
from jax.experimental import pallas as pl
from jax.experimental.pallas import tpu as pltpu
from jax.sharding import PartitionSpec as P

F32, BF16 = jnp.float32, jnp.bfloat16
MESH_ID = pl.DeviceIdType.MESH

UNIT = 256
PIECE = 64
KC = 2048
SUB = 32
WB = 256


def fused_kernel(n, x_hbm, gain, wq, wk, wv, q_out, k_out, v_out, gathered,
                 w2, acc, xt, st, ost, wst, xin, nout,
                 in_sem, wb_sem, w_sem, load_sem, out_sem,
                 own_send, own_recv, ici_send, ici_recv, d2d_send, d2d_recv):
    rows, dim = x_hbm.shape
    half = rows // 2
    n_heads, head = wq.shape[1], wq.shape[2]
    width = n_heads * head
    chips = n // 2
    nk = dim // KC
    per_half = half // PIECE
    stage_len = per_half * nk
    n_chunks = 3 * stage_len
    own_units = rows // UNIT
    n_units = n * rows // UNIT
    local_units = 2 * own_units
    n_steps = n_units * nk
    weights, outs = (wq, wk, wv), (q_out, k_out, v_out)

    me = lax.axis_index("tp")
    chip, lane = me // 2, me % 2
    sib_lane = 1 - lane
    sibling = chip * 2 + sib_lane
    ahead = (chip + 1) % chips
    behind = (chip + chips - 1) % chips
    dest = (ahead * 2 + lane, behind * 2 + lane)

    def src_row(direction, of_lane, stage, piece):
        dist = 1 + stage // 2
        if direction == 0:
            src, part = (chip + chips - dist) % chips, stage % 2
        else:
            src, part = (chip + dist) % chips, 1 - stage % 2
        return pl.multiple_of((src * 2 + of_lane) * rows + part * half + piece * PIECE, PIECE)

    def own_row(direction, stage, piece):
        part = stage % 2 if direction == 0 else 1 - stage % 2
        return pl.multiple_of(me * rows + part * half + piece * PIECE, PIECE)

    def block(row, kc):
        return gathered.at[pl.ds(row, PIECE), pl.ds(pl.multiple_of(kc * KC, KC), KC)]

    def ici_copy(direction, row, kc, m):
        return pltpu.make_async_remote_copy(
            src_ref=block(row, kc), dst_ref=block(row, kc),
            send_sem=ici_send.at[direction, m], recv_sem=ici_recv.at[direction, m],
            device_id={"tp": dest[direction]}, device_id_type=MESH_ID)

    def d2d_copy(direction, row, kc, m):
        return pltpu.make_async_remote_copy(
            src_ref=block(row, kc), dst_ref=block(row, kc),
            send_sem=d2d_send.at[direction, m], recv_sem=d2d_recv.at[direction, m],
            device_id={"tp": sibling}, device_id_type=MESH_ID)

    def own_copy(owner, idx):
        part, piece = idx % 2, idx // 2
        ref = gathered.at[pl.ds(pl.multiple_of(owner * rows + part * half + piece * PIECE, PIECE), PIECE)]
        return pltpu.make_async_remote_copy(
            src_ref=ref, dst_ref=ref, send_sem=own_send.at[idx], recv_sem=own_recv.at[idx],
            device_id={"tp": sibling}, device_id_type=MESH_ID)

    n_wb = dim // WB

    def w_copy(p, kb, slot):
        buf = (ost, wst)[slot]
        return pltpu.make_async_copy(weights[p].at[pl.ds(pl.multiple_of(kb * WB, WB), WB)], buf.at[p], w_sem.at[slot, p])

    for slot in range(2):
        for p in range(3):
            w_copy(p, slot, slot).start()

    n_pieces = rows // PIECE

    def sub_row(idx, t):
        return pl.multiple_of((idx % 2) * half + (idx // 2) * PIECE + t * SUB, SUB)

    def x_copy(idx, t):
        return pltpu.make_async_copy(x_hbm.at[pl.ds(sub_row(idx, t), SUB)], xin.at[t], in_sem.at[t])

    def n_copy(idx, t):
        row = pl.multiple_of(me * rows + sub_row(idx, t), SUB)
        return pltpu.make_async_copy(nout.at[t], gathered.at[pl.ds(row, SUB)], wb_sem.at[t])

    for t in range(2):
        x_copy(0, t).start()

    barrier = pltpu.get_barrier_semaphore()
    for peer in (dest[0], dest[1], sibling):
        pl.semaphore_signal(barrier, inc=1, device_id={"tp": peer}, device_id_type=MESH_ID)
    pl.semaphore_wait(barrier, 3)

    cw = 1024

    def normalize(t):
        for r in range(0, SUB, 16):
            sq = jnp.zeros((16, cw), F32)
            for c in range(0, dim, cw):
                xv = xin[t, r:r + 16, c:c + cw].astype(F32)
                sq = sq + xv * xv
            scale = lax.rsqrt(jnp.sum(sq, axis=-1, keepdims=True) * (1.0 / dim) + 1e-6)
            for c in range(0, dim, cw):
                xv = xin[t, r:r + 16, c:c + cw].astype(F32)
                nout[t, r:r + 16, c:c + cw] = (xv * scale * gain[:, c:c + cw]).astype(BF16)

    def send_piece(idx):
        own_copy(me, idx).start()
        piece = idx // 2
        for direction in range(2):
            @pl.when(idx % 2 == direction)
            def _():
                for kc in range(nk):
                    ici_copy(direction, own_row(direction, 0, piece), kc, piece * nk + kc).start()

    def norm_step(idx, _):
        for t in range(2):
            @pl.when(idx > 0)
            def _():
                n_copy(idx - 1, t).wait()
                if t == 1:
                    send_piece(idx - 1)

            @pl.when(idx < n_pieces)
            def _():
                x_copy(idx, t).wait()
                normalize(t)

                @pl.when(idx + 1 < n_pieces)
                def _():
                    x_copy(idx + 1, t).start()
                n_copy(idx, t).start()
        return 0

    lax.fori_loop(0, n_pieces + 1, norm_step, 0)

    def unit_rows(t, emit):
        @pl.when(t < own_units)
        def _():
            emit([pl.multiple_of(me * rows + t * UNIT + i * PIECE, PIECE) for i in range(4)])

        @pl.when(jnp.logical_and(t >= own_units, t < local_units))
        def _():
            emit([pl.multiple_of(sibling * rows + (t - own_units) * UNIT + i * PIECE, PIECE) for i in range(4)])

        @pl.when(t >= local_units)
        def _():
            u = t - local_units
            stage, piece = u // per_half, u % per_half
            emit([src_row(d, w, stage, piece) for w in (lane, sib_lane) for d in range(2)])

    def load(s, start):
        t, kc, slot = s // nk, s % nk, s % 2
        if start:
            @pl.when(jnp.logical_and(jnp.logical_and(t >= own_units, t < local_units), kc == 0))
            def _():
                for piece in range(per_half):
                    own_copy(sibling, piece * 2 + (t - own_units)).wait_recv()

            @pl.when(t >= local_units)
            def _():
                u = t - local_units
                for d in range(2):
                    d2d_copy(d, src_row(d, sib_lane, u // per_half, u % per_half), kc, u * nk + kc).wait_recv()

            def emit(row_list):
                for i, row in enumerate(row_list):
                    pltpu.make_async_copy(block(row, kc), xt.at[slot, pl.ds(i * PIECE, PIECE)], load_sem.at[slot, i]).start()
            unit_rows(t, emit)
        else:
            for i in range(4):
                pltpu.make_async_copy(block(0, 0), xt.at[slot, pl.ds(i * PIECE, PIECE)], load_sem.at[slot, i]).wait()

    def handle(m, _):
        u, kc = m // nk, m % nk
        stage, piece = u // per_half, u % per_half
        for d in range(2):
            row = src_row(d, lane, stage, piece)
            ici_copy(d, row, kc, m).wait_recv()
            d2d_copy(d, row, kc, m).start()

            @pl.when(stage == 0)
            def _():
                ici_copy(d, own_row(d, 1, piece), kc, m + stage_len).start()

            @pl.when(stage == 1)
            def _():
                ici_copy(d, src_row(d, lane, 0, piece), kc, m + stage_len).start()
        return 0

    def handled(s):
        return jnp.minimum(n_chunks, jnp.maximum(s - (local_units * nk - 2), 4 + (2 * s) // 3))

    load(0, True)

    def relayout(i, _):
        for slot in range(2):
            kb = 2 * i + slot
            buf = (ost, wst)[slot]
            for p in range(3):
                w_copy(p, kb, slot).wait()
                tmp = st.at[p % 2]
                tmp[...] = buf[p].astype(F32).reshape(WB * n_heads, head)
                for h in range(n_heads):
                    w2[pl.ds(pl.multiple_of(kb * WB, WB), WB), p * width + h * head:p * width + (h + 1) * head] = (
                        tmp[pl.ds(h, WB, stride=n_heads), :].astype(BF16))

                @pl.when(kb + 2 < n_wb)
                def _():
                    w_copy(p, kb + 2, slot).start()
        return 0

    lax.fori_loop(0, n_wb // 2, relayout, 0)

    def before(s):
        lax.fori_loop(jnp.where(s == 0, 0, handled(s - 1)), handled(s), handle, 0)

        @pl.when(s + 1 < n_steps)
        def _():
            load(s + 1, True)
        load(s, False)

    def product(s, kc, p):
        depth = pl.ds(pl.multiple_of(kc * KC, KC), KC)
        return jnp.dot(xt[s % 2], w2[depth, p * width:(p + 1) * width], preferred_element_type=F32)

    def store(t, wait):
        if wait:
            for p in range(3):
                for i in range(4):
                    pltpu.make_async_copy(ost.at[p, pl.ds(i * PIECE, PIECE)], outs[p].at[pl.ds(0, PIECE)], out_sem.at[p, i]).wait()
        else:
            def emit(row_list):
                for p in range(3):
                    for i, row in enumerate(row_list):
                        pltpu.make_async_copy(ost.at[p, pl.ds(i * PIECE, PIECE)], outs[p].at[pl.ds(row, PIECE)], out_sem.at[p, i]).start()
            unit_rows(t, emit)

    def unit(t, _):
        def partial_step(kc, _):
            s = t * nk + kc
            before(s)
            for p in range(3):
                cols = slice(p * width, (p + 1) * width)
                acc[:, cols] = jnp.where(kc == 0, 0.0, acc[:, cols]) + product(s, kc, p)
            return 0

        lax.fori_loop(0, nk - 1, partial_step, 0)
        s = t * nk + nk - 1
        before(s)

        @pl.when(t > 0)
        def _():
            store(t - 1, True)
        for p in range(3):
            total = acc[:, p * width:(p + 1) * width] + product(s, nk - 1, p)
            tmp = st.at[p % 2]
            for h in range(n_heads):
                tmp[pl.ds(h, UNIT, stride=n_heads), :] = total[:, h * head:(h + 1) * head]
            ost[p] = tmp[...].reshape(UNIT, n_heads, head).astype(BF16)
        store(t, False)
        return 0

    lax.fori_loop(0, n_units, unit, 0)
    store(n_units - 1, True)

    def drain(m, _):
        for d in range(2):
            ici_copy(d, 0, 0, m).wait_send()
            d2d_copy(d, 0, 0, m).wait_send()
        return 0

    lax.fori_loop(0, n_chunks, drain, 0)

    def drain_own(idx, _):
        own_copy(me, idx).wait_send()
        return 0

    lax.fori_loop(0, n_pieces, drain_own, 0)


def solution(mesh):
    n = mesh.shape["tp"]

    def local_step(hidden_blk, norm_gain, wq_local, wk_local, wv_local):
        rows, dim = hidden_blk.shape
        n_heads, head = wq_local.shape[1:]
        width = n_heads * head
        chunks = 3 * (rows // 2 // PIECE) * (dim // KC)
        out = jax.ShapeDtypeStruct((n * rows, n_heads, head), BF16)
        dma = pltpu.SemaphoreType.DMA
        hbm = pl.BlockSpec(memory_space=pl.ANY)
        q, k, v, _ = pl.pallas_call(
            functools.partial(fused_kernel, n),
            out_shape=(out, out, out, jax.ShapeDtypeStruct((n * rows, dim), BF16)),
            in_specs=[hbm, pl.BlockSpec(memory_space=pltpu.VMEM), hbm, hbm, hbm],
            out_specs=(hbm, hbm, hbm, hbm),
            scratch_shapes=[
                pltpu.VMEM((dim, 3 * width), BF16),
                pltpu.VMEM((UNIT, 3 * width), F32),
                pltpu.VMEM((2, UNIT, KC), BF16),
                pltpu.VMEM((2, UNIT * n_heads, head), F32),
                pltpu.VMEM((3, UNIT, n_heads, head), BF16),
                pltpu.VMEM((3, WB, n_heads, head), BF16),
                pltpu.VMEM((2, SUB, dim), BF16),
                pltpu.VMEM((2, SUB, dim), BF16),
                dma((2,)), dma((2,)), dma((2, 3)), dma((2, 4)), dma((3, 4)),
                dma((rows // PIECE,)), dma((rows // PIECE,)),
                dma((2, chunks)), dma((2, chunks)), dma((2, chunks)), dma((2, chunks)),
            ],
            compiler_params=pltpu.CompilerParams(
                collective_id=0, has_side_effects=True, vmem_limit_bytes=67043328),
            name="norm_gather_project",
        )(hidden_blk, norm_gain.reshape(1, dim), wq_local, wk_local, wv_local)
        return q, k, v

    row_spec = P(("dp", "tp"), None)
    head_spec = P(None, "tp", None)
    out_spec = P("dp", "tp", None)
    return jax.shard_map(local_step, mesh=mesh, in_specs=(row_spec, P(None), head_spec, head_spec, head_spec), out_specs=(out_spec, out_spec, out_spec), check_vma=False)
```

```python
import functools

import jax
import jax.numpy as jnp
from jax import lax
from jax.experimental import pallas as pl
from jax.experimental.pallas import tpu as pltpu
from jax.sharding import PartitionSpec as P

F32, BF16 = jnp.float32, jnp.bfloat16
MESH_ID = pl.DeviceIdType.MESH

UNIT = 256
PIECE = 64
KC = 2048
SUB = 32
WB = 256


def fused_kernel(n, x_hbm, gain, wq, wk, wv, q_out, k_out, v_out, gathered, w2,
                 acc, xt, st, ost, wst, xin, nout,
                 in_sem, wb_sem, w_sem, load_sem, out_sem,
                 own_send, own_recv, ici_send, ici_recv, d2d_send, d2d_recv):
    rows, dim = x_hbm.shape
    half = rows // 2
    n_heads, head = wq.shape[1], wq.shape[2]
    width = n_heads * head
    chips = n // 2
    nk = dim // KC
    per_half = half // PIECE
    stage_len = per_half * nk
    n_chunks = 3 * stage_len
    own_units = rows // UNIT
    n_units = n * rows // UNIT - 1
    local_units = 2 * own_units
    n_steps = n_units * nk
    weights, outs = (wq, wk, wv), (q_out, k_out, v_out)

    me = lax.axis_index("tp")
    chip, lane = me // 2, me % 2
    sib_lane = 1 - lane
    sibling = chip * 2 + sib_lane
    ahead = (chip + 1) % chips
    behind = (chip + chips - 1) % chips
    dest = (ahead * 2 + lane, behind * 2 + lane)

    def src_row(direction, of_lane, stage, piece):
        dist = 1 + stage // 2
        if direction == 0:
            src, part = (chip + chips - dist) % chips, stage % 2
        else:
            src, part = (chip + dist) % chips, 1 - stage % 2
        return pl.multiple_of((src * 2 + of_lane) * rows + part * half + piece * PIECE, PIECE)

    def own_row(direction, stage, piece):
        part = stage % 2 if direction == 0 else 1 - stage % 2
        return pl.multiple_of(me * rows + part * half + piece * PIECE, PIECE)

    def block(row, kc):
        return gathered.at[pl.ds(row, PIECE), pl.ds(pl.multiple_of(kc * KC, KC), KC)]

    def ici_copy(direction, row, kc, m):
        return pltpu.make_async_remote_copy(
            src_ref=block(row, kc), dst_ref=block(row, kc),
            send_sem=ici_send.at[direction, m], recv_sem=ici_recv.at[direction, m],
            device_id={"tp": dest[direction]}, device_id_type=MESH_ID)

    def d2d_copy(direction, row, kc, m):
        return pltpu.make_async_remote_copy(
            src_ref=block(row, kc), dst_ref=block(row, kc),
            send_sem=d2d_send.at[direction, m], recv_sem=d2d_recv.at[direction, m],
            device_id={"tp": sibling}, device_id_type=MESH_ID)

    def own_copy(owner, idx):
        part, piece = idx % 2, idx // 2
        ref = gathered.at[pl.ds(pl.multiple_of(owner * rows + part * half + piece * PIECE, PIECE), PIECE)]
        return pltpu.make_async_remote_copy(
            src_ref=ref, dst_ref=ref, send_sem=own_send.at[idx], recv_sem=own_recv.at[idx],
            device_id={"tp": sibling}, device_id_type=MESH_ID)

    n_wb = dim // WB

    def w_copy(p, kb, slot):
        buf = (ost, wst)[slot]
        return pltpu.make_async_copy(weights[p].at[pl.ds(pl.multiple_of(kb * WB, WB), WB)], buf.at[p], w_sem.at[slot, p])

    n_pieces = rows // PIECE

    def sub_row(idx, t):
        return pl.multiple_of((idx % 2) * half + (idx // 2) * PIECE + t * SUB, SUB)

    def x_copy(idx, t):
        return pltpu.make_async_copy(x_hbm.at[pl.ds(sub_row(idx, t), SUB)], xin.at[t], in_sem.at[t])

    def n_copy(idx, t):
        row = pl.multiple_of(me * rows + sub_row(idx, t), SUB)
        return pltpu.make_async_copy(nout.at[t], gathered.at[pl.ds(row, SUB)], wb_sem.at[t])

    for t in range(2):
        x_copy(0, t).start()
    for slot in range(2):
        for p in range(3):
            w_copy(p, slot, slot).start()

    barrier = pltpu.get_barrier_semaphore()
    for peer in (dest[0], dest[1], sibling):
        pl.semaphore_signal(barrier, inc=1, device_id={"tp": peer}, device_id_type=MESH_ID)
    pl.semaphore_wait(barrier, 3)

    cw = 1024

    def normalize(t):
        for r in range(0, SUB, 16):
            sq = jnp.zeros((16, cw), F32)
            for c in range(0, dim, cw):
                xv = xin[t, r:r + 16, c:c + cw].astype(F32)
                sq = sq + xv * xv
            scale = lax.rsqrt(jnp.sum(sq, axis=-1, keepdims=True) * (1.0 / dim) + 1e-6)
            for c in range(0, dim, cw):
                xv = xin[t, r:r + 16, c:c + cw].astype(F32)
                nout[t, r:r + 16, c:c + cw] = (xv * scale * gain[:, c:c + cw]).astype(BF16)

    def send_piece(idx):
        own_copy(me, idx).start()
        piece = idx // 2
        for direction in range(2):
            @pl.when(idx % 2 == direction)
            def _():
                for kc in range(nk):
                    ici_copy(direction, own_row(direction, 0, piece), kc, piece * nk + kc).start()

    def norm_step(idx, _):
        for t in range(2):
            @pl.when(idx > 0)
            def _():
                n_copy(idx - 1, t).wait()
                if t == 1:
                    send_piece(idx - 1)

            @pl.when(idx < n_pieces)
            def _():
                x_copy(idx, t).wait()
                normalize(t)

                @pl.when(idx + 1 < n_pieces)
                def _():
                    x_copy(idx + 1, t).start()
                n_copy(idx, t).start()
        return 0

    lax.fori_loop(0, n_pieces + 1, norm_step, 0)

    def unit_rows(t, emit):
        @pl.when(t < own_units)
        def _():
            emit([pl.multiple_of(me * rows + t * UNIT + i * PIECE, PIECE) for i in range(4)])

        @pl.when(jnp.logical_and(t >= own_units, t < local_units))
        def _():
            emit([pl.multiple_of(sibling * rows + (t - own_units) * UNIT + i * PIECE, PIECE) for i in range(4)])

        @pl.when(t >= local_units)
        def _():
            u = t - local_units
            stage, piece = u // per_half, u % per_half
            emit([src_row(d, w, stage, piece) for w in (lane, sib_lane) for d in range(2)])

    def load(s, start):
        t, kc, slot = s // nk, s % nk, s % 2
        if start:
            @pl.when(jnp.logical_and(jnp.logical_and(t >= own_units, t < local_units), kc == 0))
            def _():
                for piece in range(per_half):
                    own_copy(sibling, piece * 2 + (t - own_units)).wait_recv()

            @pl.when(t >= local_units)
            def _():
                u = t - local_units
                for d in range(2):
                    d2d_copy(d, src_row(d, sib_lane, u // per_half, u % per_half), kc, u * nk + kc).wait_recv()

            def emit(row_list):
                for i, row in enumerate(row_list):
                    pltpu.make_async_copy(block(row, kc), xt.at[slot, pl.ds(i * PIECE, PIECE)], load_sem.at[slot, i]).start()
            unit_rows(t, emit)
        else:
            for i in range(4):
                pltpu.make_async_copy(block(0, 0), xt.at[slot, pl.ds(i * PIECE, PIECE)], load_sem.at[slot, i]).wait()

    def handle(m, _):
        u, kc = m // nk, m % nk
        stage, piece = u // per_half, u % per_half
        for d in range(2):
            row = src_row(d, lane, stage, piece)
            ici_copy(d, row, kc, m).wait_recv()
            d2d_copy(d, row, kc, m).start()

            @pl.when(stage == 0)
            def _():
                ici_copy(d, own_row(d, 1, piece), kc, m + stage_len).start()

            @pl.when(stage == 1)
            def _():
                ici_copy(d, src_row(d, lane, 0, piece), kc, m + stage_len).start()
        return 0

    def handled(s):
        return jnp.minimum(n_chunks - nk, jnp.maximum(s - (local_units * nk - 2), 4 + (2 * s) // 3))

    load(0, True)

    def relayout(i, _):
        for slot in range(2):
            kb = 2 * i + slot
            buf = (ost, wst)[slot]
            for p in range(3):
                w_copy(p, kb, slot).wait()
                tmp = st.at[p % 2]
                tmp[...] = buf[p].astype(F32).reshape(WB * n_heads, head)
                for h in range(n_heads):
                    w2[pl.ds(pl.multiple_of(kb * WB, WB), WB), p * width + h * head:p * width + (h + 1) * head] = (
                        tmp[pl.ds(h, WB, stride=n_heads), :].astype(BF16))

                @pl.when(kb + 2 < n_wb)
                def _():
                    w_copy(p, kb + 2, slot).start()
        return 0

    lax.fori_loop(0, n_wb // 2, relayout, 0)

    def before(s):
        lax.fori_loop(jnp.where(s == 0, 0, handled(s - 1)), handled(s), handle, 0)

        @pl.when(s + 1 < n_steps)
        def _():
            load(s + 1, True)
        load(s, False)

    def product(s, kc, p):
        depth = pl.ds(pl.multiple_of(kc * KC, KC), KC)
        return jnp.dot(xt[s % 2], w2[depth, p * width:(p + 1) * width], preferred_element_type=F32)

    def store(t, wait):
        if wait:
            for p in range(3):
                for i in range(4):
                    pltpu.make_async_copy(ost.at[p, pl.ds(i * PIECE, PIECE)], outs[p].at[pl.ds(0, PIECE)], out_sem.at[p, i]).wait()
        else:
            def emit(row_list):
                for p in range(3):
                    for i, row in enumerate(row_list):
                        pltpu.make_async_copy(ost.at[p, pl.ds(i * PIECE, PIECE)], outs[p].at[pl.ds(row, PIECE)], out_sem.at[p, i]).start()
            unit_rows(t, emit)

    def unit(t, _):
        def partial_step(kc, _):
            s = t * nk + kc
            before(s)
            for p in range(3):
                cols = slice(p * width, (p + 1) * width)
                acc[:, cols] = jnp.where(kc == 0, 0.0, acc[:, cols]) + product(s, kc, p)
            return 0

        lax.fori_loop(0, nk - 1, partial_step, 0)
        s = t * nk + nk - 1
        before(s)

        @pl.when(t > 0)
        def _():
            store(t - 1, True)
        for p in range(3):
            total = acc[:, p * width:(p + 1) * width] + product(s, nk - 1, p)
            tmp = st.at[p % 2]
            for h in range(n_heads):
                tmp[pl.ds(h, UNIT, stride=n_heads), :] = total[:, h * head:(h + 1) * head]
            ost[p] = tmp[...].reshape(UNIT, n_heads, head).astype(BF16)
        store(t, False)
        return 0

    lax.fori_loop(0, n_units, unit, 0)
    store(n_units - 1, True)

    lax.fori_loop(n_chunks - nk, n_chunks, handle, 0)
    for kc in range(nk):
        for d in range(2):
            d2d_copy(d, src_row(d, sib_lane, 2, per_half - 1), kc, n_chunks - nk + kc).wait_recv()

    def drain(m, _):
        for d in range(2):
            ici_copy(d, 0, 0, m).wait_send()
            d2d_copy(d, 0, 0, m).wait_send()
        return 0

    lax.fori_loop(0, n_chunks, drain, 0)

    def drain_own(idx, _):
        own_copy(me, idx).wait_send()
        return 0

    lax.fori_loop(0, n_pieces, drain_own, 0)


def finish_kernel(n, w2, gathered, q_in, k_in, v_in, q_out, k_out, v_out,
                  acc, xt, st, ost, buf, load_sem, read_sem, write_sem, out_sem):
    ins, outs = (q_in, k_in, v_in), (q_out, k_out, v_out)
    total_rows, dim = gathered.shape
    rows = total_rows // n
    half = rows // 2
    n_heads, head = q_in.shape[1], q_in.shape[2]
    width = n_heads * head
    chips = n // 2
    nk = dim // KC
    chip_rows = 2 * rows

    far = (lax.axis_index("tp") // 2 + chips // 2) % chips
    unit_rows = [pl.multiple_of(far * chip_rows + end - PIECE, PIECE) for end in range(half, chip_rows + 1, half)]
    moves = []
    for other in range(1, chips):
        base = ((far + other) % chips) * chip_rows
        moves += [(pl.multiple_of(base + r, UNIT), UNIT) for r in range(0, chip_rows, UNIT)]
    moves += [(pl.multiple_of(far * chip_rows + r, UNIT), half - PIECE) for r in range(0, chip_rows, half)]

    def read(j):
        row, size = moves[j]
        return [pltpu.make_async_copy(ins[p].at[pl.ds(row, size)], buf.at[j % 3, p, pl.ds(0, size)], read_sem.at[j % 3, p]) for p in range(3)]

    def write(j):
        row, size = moves[j]
        return [pltpu.make_async_copy(buf.at[j % 3, p, pl.ds(0, size)], outs[p].at[pl.ds(row, size)], write_sem.at[j % 3, p]) for p in range(3)]

    def tick(j):
        if 0 <= j - 3 < len(moves):
            for c in write(j - 3):
                c.wait()
        if 0 <= j < len(moves):
            for c in read(j):
                c.start()
        if 0 <= j - 1 < len(moves):
            for c in read(j - 1):
                c.wait()
            for c in write(j - 1):
                c.start()

    def load(kc):
        return [pltpu.make_async_copy(
            gathered.at[pl.ds(row, PIECE), pl.ds(kc * KC, KC)], xt.at[kc % 2, pl.ds(i * PIECE, PIECE)], load_sem.at[kc % 2, i])
            for i, row in enumerate(unit_rows)]

    def result(p):
        return [pltpu.make_async_copy(ost.at[p, pl.ds(i * PIECE, PIECE)], outs[p].at[pl.ds(row, PIECE)], out_sem.at[p, i])
                for i, row in enumerate(unit_rows)]

    for kc in range(min(2, nk)):
        for c in load(kc):
            c.start()
    ticks = len(moves) + 3
    done = 2
    for j in range(done):
        tick(j)
    n_dots = 3 * nk
    for kc in range(nk):
        for c in load(kc):
            c.wait()
        for p in range(3):
            cols = slice(p * width, (p + 1) * width)
            part = jnp.dot(xt[kc % 2], w2[kc * KC:(kc + 1) * KC, cols], preferred_element_type=F32)
            if kc > 0:
                part = acc[:, cols] + part
            if kc < nk - 1:
                acc[:, cols] = part
            else:
                tmp = st.at[p % 2]
                for h in range(n_heads):
                    tmp[pl.ds(h, UNIT, stride=n_heads), :] = part[:, h * head:(h + 1) * head]
                ost[p] = tmp[...].reshape(UNIT, n_heads, head).astype(BF16)
                for c in result(p):
                    c.start()
            upto = 2 + (kc * 3 + p + 1) * (ticks - 3) // n_dots
            for j in range(done, upto):
                tick(j)
            done = upto
        if kc + 2 < nk:
            for c in load(kc + 2):
                c.start()
    for j in range(done, ticks):
        tick(j)
    for p in range(3):
        for c in result(p):
            c.wait()


def solution(mesh):
    n = mesh.shape["tp"]

    def local_step(hidden_blk, norm_gain, wq_local, wk_local, wv_local):
        rows, dim = hidden_blk.shape
        n_heads, head = wq_local.shape[1:]
        width = n_heads * head
        chunks = 3 * (rows // 2 // PIECE) * (dim // KC)
        out = jax.ShapeDtypeStruct((n * rows, n_heads, head), BF16)
        dma = pltpu.SemaphoreType.DMA
        hbm = pl.BlockSpec(memory_space=pl.ANY)
        vmem = pl.BlockSpec(memory_space=pltpu.VMEM)
        room = 67043328 - 2 * dim * 3 * width
        q, k, v, gathered, w2 = pl.pallas_call(
            functools.partial(fused_kernel, n),
            out_shape=(out, out, out, jax.ShapeDtypeStruct((n * rows, dim), BF16), pltpu.VMEM((dim, 3 * width), BF16)),
            in_specs=[hbm, vmem, hbm, hbm, hbm],
            out_specs=(hbm, hbm, hbm, hbm, vmem),
            scratch_shapes=[
                pltpu.VMEM((UNIT, 3 * width), F32),
                pltpu.VMEM((2, UNIT, KC), BF16),
                pltpu.VMEM((2, UNIT * n_heads, head), F32),
                pltpu.VMEM((3, UNIT, n_heads, head), BF16),
                pltpu.VMEM((3, WB, n_heads, head), BF16),
                pltpu.VMEM((2, SUB, dim), BF16),
                pltpu.VMEM((2, SUB, dim), BF16),
                dma((2,)), dma((2,)), dma((2, 3)), dma((2, 4)), dma((3, 4)),
                dma((rows // PIECE,)), dma((rows // PIECE,)),
                dma((2, chunks)), dma((2, chunks)), dma((2, chunks)), dma((2, chunks)),
            ],
            compiler_params=pltpu.CompilerParams(
                collective_id=0, has_side_effects=True, vmem_limit_bytes=room),
            name="norm_gather_project",
        )(hidden_blk, norm_gain.reshape(1, dim), wq_local, wk_local, wv_local)
        return pl.pallas_call(
            functools.partial(finish_kernel, n),
            out_shape=(out, out, out),
            in_specs=[vmem, hbm, hbm, hbm, hbm],
            out_specs=(hbm, hbm, hbm),
            scratch_shapes=[
                pltpu.VMEM((UNIT, 3 * width), F32),
                pltpu.VMEM((2, UNIT, KC), BF16),
                pltpu.VMEM((2, UNIT * n_heads, head), F32),
                pltpu.VMEM((3, UNIT, n_heads, head), BF16),
                pltpu.VMEM((3, 3, UNIT, n_heads, head), BF16),
                dma((2, 4)), dma((3, 3)), dma((3, 3)), dma((3, 4)),
            ],
            compiler_params=pltpu.CompilerParams(vmem_limit_bytes=room),
            name="finish",
        )(pltpu.with_memory_space_constraint(w2, pltpu.VMEM), gathered, q, k, v)

    row_spec = P(("dp", "tp"), None)
    head_spec = P(None, "tp", None)
    out_spec = P("dp", "tp", None)
    return jax.shard_map(local_step, mesh=mesh, in_specs=(row_spec, P(None), head_spec, head_spec, head_spec), out_specs=(out_spec, out_spec, out_spec), check_vma=False)
```

```python
import functools

import jax
import jax.numpy as jnp
from jax import lax
from jax.experimental import pallas as pl
from jax.experimental.pallas import tpu as pltpu
from jax.sharding import PartitionSpec as P

F32, BF16 = jnp.float32, jnp.bfloat16
MESH_ID = pl.DeviceIdType.MESH

UNIT = 256
PIECE = 64
KC = 2048
SLOTS = 10
SPAN = 128
FIRST_READS = 3
SUB = 32
WB = 256


def fused_kernel(n, x_hbm, gain, wq, wk, wv, q_out, k_out, v_out, gathered, w2,
                 acc, xt, st, ost, wst, xin,
                 in_sem, wb_sem, w_sem, load_sem, out_sem,
                 own_send, own_recv, ici_send, ici_recv, d2d_send, d2d_recv):
    rows, dim = x_hbm.shape
    half = rows // 2
    n_heads, head = wq.shape[1], wq.shape[2]
    width = n_heads * head
    chips = n // 2
    nk = dim // KC
    per_half = half // PIECE
    stage_len = per_half * nk
    n_chunks = 3 * stage_len
    own_units = rows // UNIT
    n_units = n * rows // UNIT - 1
    local_units = 2 * own_units
    n_steps = n_units * nk
    weights, outs = (wq, wk, wv), (q_out, k_out, v_out)

    me = lax.axis_index("tp")
    chip, lane = me // 2, me % 2
    sib_lane = 1 - lane
    sibling = chip * 2 + sib_lane
    ahead = (chip + 1) % chips
    behind = (chip + chips - 1) % chips
    dest = (ahead * 2 + lane, behind * 2 + lane)

    def src_row(direction, of_lane, stage, piece):
        dist = 1 + stage // 2
        if direction == 0:
            src, part = (chip + chips - dist) % chips, stage % 2
        else:
            src, part = (chip + dist) % chips, 1 - stage % 2
        return pl.multiple_of((src * 2 + of_lane) * rows + part * half + piece * PIECE, PIECE)

    def own_row(direction, stage, piece):
        part = stage % 2 if direction == 0 else 1 - stage % 2
        return pl.multiple_of(me * rows + part * half + piece * PIECE, PIECE)

    def block(row, kc):
        return gathered.at[pl.ds(row, PIECE), pl.ds(pl.multiple_of(kc * KC, KC), KC)]

    def ici_copy(direction, row, kc, m):
        return pltpu.make_async_remote_copy(
            src_ref=block(row, kc), dst_ref=block(row, kc),
            send_sem=ici_send.at[direction, m], recv_sem=ici_recv.at[direction, m],
            device_id={"tp": dest[direction]}, device_id_type=MESH_ID)

    def d2d_copy(direction, row, kc, m):
        return pltpu.make_async_remote_copy(
            src_ref=block(row, kc), dst_ref=block(row, kc),
            send_sem=d2d_send.at[direction, m], recv_sem=d2d_recv.at[direction, m],
            device_id={"tp": sibling}, device_id_type=MESH_ID)

    def own_copy(owner, idx):
        part, piece = idx % 2, idx // 2
        ref = gathered.at[pl.ds(pl.multiple_of(owner * rows + part * half + piece * PIECE, PIECE), PIECE)]
        return pltpu.make_async_remote_copy(
            src_ref=ref, dst_ref=ref, send_sem=own_send.at[idx], recv_sem=own_recv.at[idx],
            device_id={"tp": sibling}, device_id_type=MESH_ID)

    n_wb = dim // WB

    def w_copy(p, kb, slot):
        buf = (ost, wst)[slot]
        return pltpu.make_async_copy(weights[p].at[pl.ds(pl.multiple_of(kb * WB, WB), WB)], buf.at[p], w_sem.at[slot, p])

    n_pieces = rows // PIECE

    def sub_row(idx, t):
        return pl.multiple_of((idx % 2) * half + (idx // 2) * PIECE + t * SUB, SUB)

    def x_copy(idx, t):
        slot = (idx % 2) * 2 + t
        return pltpu.make_async_copy(x_hbm.at[pl.ds(sub_row(idx, t), SUB)], xin.at[slot], in_sem.at[slot])

    def n_copies(idx, t):
        row = pl.multiple_of(me * rows + sub_row(idx, t), SUB)
        return [pltpu.make_async_copy(
            xt.at[idx % 2, pl.ds((t * nk + kc) * SUB, SUB)],
            gathered.at[pl.ds(row, SUB), pl.ds(kc * KC, KC)], wb_sem.at[(idx % 2) * 2 + t, kc]) for kc in range(nk)]

    for idx in range(2):
        for t in range(2):
            x_copy(idx, t).start()
    for slot in range(2):
        for p in range(3):
            w_copy(p, slot, slot).start()

    barrier = pltpu.get_barrier_semaphore()
    for peer in (dest[0], dest[1], sibling):
        pl.semaphore_signal(barrier, inc=1, device_id={"tp": peer}, device_id_type=MESH_ID)
    pl.semaphore_wait(barrier, 3)

    cw = min(1024, KC)

    def normalize(idx, t):
        slot = (idx % 2) * 2 + t
        for r in range(0, SUB, 16):
            sq = jnp.zeros((16, cw), F32)
            for c in range(0, dim, cw):
                xv = xin[slot, r:r + 16, c:c + cw].astype(F32)
                sq = sq + xv * xv
            scale = lax.rsqrt(jnp.sum(sq, axis=-1, keepdims=True) * (1.0 / dim) + 1e-6)
            for c in range(0, dim, cw):
                xv = xin[slot, r:r + 16, c:c + cw].astype(F32)
                first = (t * nk + c // KC) * SUB + r
                xt[idx % 2, first:first + 16, c % KC:c % KC + cw] = (xv * scale * gain[:, c:c + cw]).astype(BF16)

    def send_piece(idx):
        piece = idx // 2
        for direction in range(2):
            @pl.when(idx % 2 == direction)
            def _():
                for kc in range(nk):
                    ici_copy(direction, own_row(direction, 0, piece), kc, piece * nk + kc).start()
        own_copy(me, idx).start()

    def norm_step(idx, _):
        for t in range(2):
            @pl.when(idx < n_pieces)
            def _():
                x_copy(idx, t).wait()
                normalize(idx, t)

                @pl.when(idx + 2 < n_pieces)
                def _():
                    x_copy(idx + 2, t).start()
                for c in n_copies(idx, t):
                    c.start()

            if t == 0:
                @pl.when(idx > 0)
                def _():
                    for u in range(2):
                        for c in n_copies(idx - 1, u):
                            c.wait()
                    send_piece(idx - 1)
        return 0

    lax.fori_loop(0, n_pieces + 1, norm_step, 0)

    def unit_rows(t, emit):
        @pl.when(t < own_units)
        def _():
            emit([pl.multiple_of(me * rows + t * UNIT + i * PIECE, PIECE) for i in range(4)])

        @pl.when(jnp.logical_and(t >= own_units, t < local_units))
        def _():
            emit([pl.multiple_of(sibling * rows + (t - own_units) * UNIT + i * PIECE, PIECE) for i in range(4)])

        @pl.when(t >= local_units)
        def _():
            u = t - local_units
            stage, piece = u // per_half, u % per_half
            emit([src_row(d, w, stage, piece) for w in (lane, sib_lane) for d in range(2)])

    def load(s, start):
        t, kc, slot = s // nk, s % nk, s % 2
        if start:
            @pl.when(jnp.logical_and(jnp.logical_and(t >= own_units, t < local_units), kc == 0))
            def _():
                for piece in range(per_half):
                    own_copy(sibling, piece * 2 + (t - own_units)).wait_recv()

            @pl.when(t >= local_units)
            def _():
                u = t - local_units
                for d in range(2):
                    d2d_copy(d, src_row(d, sib_lane, u // per_half, u % per_half), kc, u * nk + kc).wait_recv()

            def emit(row_list):
                for i, row in enumerate(row_list):
                    pltpu.make_async_copy(block(row, kc), xt.at[slot, pl.ds(i * PIECE, PIECE)], load_sem.at[slot, i]).start()
            unit_rows(t, emit)
        else:
            for i in range(4):
                pltpu.make_async_copy(block(0, 0), xt.at[slot, pl.ds(i * PIECE, PIECE)], load_sem.at[slot, i]).wait()

    def handle(m, _):
        u, kc = m // nk, m % nk
        stage, piece = u // per_half, u % per_half
        for d in range(2):
            row = src_row(d, lane, stage, piece)
            ici_copy(d, row, kc, m).wait_recv()
            d2d_copy(d, row, kc, m).start()

            @pl.when(stage == 0)
            def _():
                ici_copy(d, own_row(d, 1, piece), kc, m + stage_len).start()

            @pl.when(stage == 1)
            def _():
                ici_copy(d, src_row(d, lane, 0, piece), kc, m + stage_len).start()
        return 0

    def handled(s):
        return jnp.minimum(n_chunks - nk, jnp.maximum(s - (local_units * nk - 2), 4 + (2 * s) // 3))

    load(0, True)

    def relayout(i, _):
        for slot in range(2):
            kb = 2 * i + slot
            buf = (ost, wst)[slot]
            for p in range(3):
                w_copy(p, kb, slot).wait()
                tmp = st.at[p % 2]
                tmp[...] = buf[p].astype(F32).reshape(WB * n_heads, head)
                for h in range(n_heads):
                    w2[pl.ds(pl.multiple_of(kb * WB, WB), WB), p * width + h * head:p * width + (h + 1) * head] = (
                        tmp[pl.ds(h, WB, stride=n_heads), :].astype(BF16))

                @pl.when(kb + 2 < n_wb)
                def _():
                    w_copy(p, kb + 2, slot).start()
        return 0

    lax.fori_loop(0, n_wb // 2, relayout, 0)

    def before(s):
        lax.fori_loop(jnp.where(s == 0, 0, handled(s - 1)), handled(s), handle, 0)

        @pl.when(s + 1 < n_steps)
        def _():
            load(s + 1, True)
        load(s, False)

    def product(s, kc, p):
        depth = pl.ds(pl.multiple_of(kc * KC, KC), KC)
        return jnp.dot(xt[s % 2], w2[depth, p * width:(p + 1) * width], preferred_element_type=F32)

    def store(t, wait):
        if wait:
            for p in range(3):
                for i in range(4):
                    pltpu.make_async_copy(ost.at[p, pl.ds(i * PIECE, PIECE)], outs[p].at[pl.ds(0, PIECE)], out_sem.at[p, i]).wait()
        else:
            def emit(row_list):
                for p in range(3):
                    for i, row in enumerate(row_list):
                        pltpu.make_async_copy(ost.at[p, pl.ds(i * PIECE, PIECE)], outs[p].at[pl.ds(row, PIECE)], out_sem.at[p, i]).start()
            unit_rows(t, emit)

    def unit(t, _):
        def partial_step(kc, _):
            s = t * nk + kc
            before(s)
            for p in range(3):
                cols = slice(p * width, (p + 1) * width)
                acc[:, cols] = jnp.where(kc == 0, 0.0, acc[:, cols]) + product(s, kc, p)
            return 0

        lax.fori_loop(0, nk - 1, partial_step, 0)
        s = t * nk + nk - 1
        before(s)

        @pl.when(t > 0)
        def _():
            store(t - 1, True)
        for p in range(3):
            total = acc[:, p * width:(p + 1) * width] + product(s, nk - 1, p)
            tmp = st.at[p % 2]
            for h in range(n_heads):
                tmp[pl.ds(h, UNIT, stride=n_heads), :] = total[:, h * head:(h + 1) * head]
            ost[p] = tmp[...].reshape(UNIT, n_heads, head).astype(BF16)
        store(t, False)
        return 0

    lax.fori_loop(0, n_units, unit, 0)
    store(n_units - 1, True)

    def drain(m, _):
        for d in range(2):
            ici_copy(d, 0, 0, m).wait_send()
            d2d_copy(d, 0, 0, m).wait_send()
        return 0

    def drain_own(idx, _):
        own_copy(me, idx).wait_send()
        return 0

    lax.fori_loop(0, n_pieces, drain_own, 0)
    lax.fori_loop(0, n_chunks - nk, drain, 0)

    lax.fori_loop(n_chunks - nk, n_chunks, handle, 0)
    lax.fori_loop(n_chunks - nk, n_chunks, drain, 0)
    for kc in range(nk):
        for d in range(2):
            d2d_copy(d, src_row(d, sib_lane, 2, per_half - 1), kc, n_chunks - nk + kc).wait_recv()


def finish_kernel(n, w2, gathered, q_in, k_in, v_in, q_out, k_out, v_out,
                  xt, acc, st, ost, buf, load_sem, read_sem, write_sem, out_sem):
    ins, outs = (q_in, k_in, v_in), (q_out, k_out, v_out)
    total_rows, dim = gathered.shape
    rows = total_rows // n
    half = rows // 2
    n_heads, head = q_in.shape[1], q_in.shape[2]
    width = n_heads * head
    chips = n // 2
    chip_rows = 2 * rows
    slots, span = buf.shape[0], buf.shape[2]

    far = (lax.axis_index("tp") // 2 + chips // 2) % chips
    unit_rows = [pl.multiple_of(far * chip_rows + end - PIECE, PIECE) for end in range(half, chip_rows + 1, half)]
    moves = []
    for other in range(1, chips):
        base = ((far + other) % chips) * chip_rows
        moves += [(pl.multiple_of(base + r, PIECE), span) for r in range(0, chip_rows, span)]
    for part in range(0, chip_rows, half):
        for r in range(0, half - PIECE, span):
            moves.append((pl.multiple_of(far * chip_rows + part + r, PIECE), min(span, half - PIECE - r)))

    def read(j):
        row, size = moves[j]
        return [pltpu.make_async_copy(ins[p].at[pl.ds(row, size)], buf.at[j % slots, p, pl.ds(0, size)], read_sem.at[j % slots, p]) for p in range(3)]

    def write(j):
        row, size = moves[j]
        return [pltpu.make_async_copy(buf.at[j % slots, p, pl.ds(0, size)], outs[p].at[pl.ds(row, size)], write_sem.at[j % slots, p]) for p in range(3)]

    def start(copies):
        for c in copies:
            c.start()

    def wait(copies):
        for c in copies:
            c.wait()

    deep = dim // 2

    def loads(k):
        return [pltpu.make_async_copy(
            gathered.at[pl.ds(row, PIECE), pl.ds(k * deep, deep)],
            xt.at[pl.ds(i * PIECE, PIECE), pl.ds(k * deep, deep)], load_sem.at[k, i]) for i, row in enumerate(unit_rows)]

    def result(p):
        return [pltpu.make_async_copy(ost.at[p, pl.ds(i * PIECE, PIECE)], outs[p].at[pl.ds(row, PIECE)], out_sem.at[p, i])
                for i, row in enumerate(unit_rows)]

    n_read, n_written, n_freed = 0, 0, 0
    for k in range(2):
        start(loads(k))
    for _ in range(FIRST_READS):
        start(read(n_read))
        n_read += 1
    wait(loads(0))
    while n_read < slots:
        start(read(n_read))
        n_read += 1

    n_cols = acc.shape[1]
    n_dots = 2 * (3 * width // n_cols)
    per_p = width // n_cols
    heads = n_cols // head
    for i_dot in range(n_dots):
        nb, k = i_dot // 2, i_dot % 2
        if i_dot == 1:
            wait(loads(1))
        part = jnp.dot(xt[:, k * deep:(k + 1) * deep], w2[k * deep:(k + 1) * deep, nb * n_cols:(nb + 1) * n_cols],
                       preferred_element_type=F32)
        if k == 0:
            acc[...] = part
        else:
            part = acc[...] + part
            p = nb // per_p
            for i in range(heads):
                st[pl.ds((nb % per_p) * heads + i, UNIT, stride=n_heads), :] = part[:, i * head:(i + 1) * head]
            if nb % per_p == per_p - 1:
                ost[p] = st[...].reshape(UNIT, n_heads, head).astype(BF16)
                start(result(p))
        free = n_written
        target = min(len(moves), -(-len(moves) * (i_dot + 1) // (n_dots - 1)))
        while n_written < min(target, n_read):
            wait(read(n_written))
            start(write(n_written))
            n_written += 1
        while n_freed < free:
            wait(write(n_freed))
            n_freed += 1
            if n_read < len(moves):
                start(read(n_read))
                n_read += 1
    while n_written < len(moves):
        while n_freed < n_written and n_read < len(moves):
            wait(write(n_freed))
            n_freed += 1
            start(read(n_read))
            n_read += 1
        wait(read(n_written))
        start(write(n_written))
        n_written += 1
    while n_freed < len(moves):
        wait(write(n_freed))
        n_freed += 1
    for p in range(3):
        wait(result(p))


def solution(mesh):
    n = mesh.shape["tp"]

    def local_step(hidden_blk, norm_gain, wq_local, wk_local, wv_local):
        rows, dim = hidden_blk.shape
        n_heads, head = wq_local.shape[1:]
        width = n_heads * head
        chunks = 3 * (rows // 2 // PIECE) * (dim // KC)
        out = jax.ShapeDtypeStruct((n * rows, n_heads, head), BF16)
        dma = pltpu.SemaphoreType.DMA
        hbm = pl.BlockSpec(memory_space=pl.ANY)
        vmem = pl.BlockSpec(memory_space=pltpu.VMEM)
        room = 67043328 - 2 * dim * 3 * width
        q, k, v, gathered, w2 = pl.pallas_call(
            functools.partial(fused_kernel, n),
            out_shape=(out, out, out, jax.ShapeDtypeStruct((n * rows, dim), BF16), pltpu.VMEM((dim, 3 * width), BF16)),
            in_specs=[hbm, vmem, hbm, hbm, hbm],
            out_specs=(hbm, hbm, hbm, hbm, vmem),
            scratch_shapes=[
                pltpu.VMEM((UNIT, 3 * width), F32),
                pltpu.VMEM((2, UNIT, KC), BF16),
                pltpu.VMEM((2, UNIT * n_heads, head), F32),
                pltpu.VMEM((3, UNIT, n_heads, head), BF16),
                pltpu.VMEM((3, WB, n_heads, head), BF16),
                pltpu.VMEM((4, SUB, dim), BF16),
                dma((4,)), dma((4, dim // KC)), dma((2, 3)), dma((2, 4)), dma((3, 4)),
                dma((rows // PIECE,)), dma((rows // PIECE,)),
                dma((2, chunks)), dma((2, chunks)), dma((2, chunks)), dma((2, chunks)),
            ],
            compiler_params=pltpu.CompilerParams(
                collective_id=0, has_side_effects=True, vmem_limit_bytes=room),
            name="norm_gather_project",
        )(hidden_blk, norm_gain.reshape(1, dim), wq_local, wk_local, wv_local)
        return pl.pallas_call(
            functools.partial(finish_kernel, n),
            out_shape=(out, out, out),
            in_specs=[vmem, hbm, hbm, hbm, hbm],
            out_specs=(hbm, hbm, hbm),
            scratch_shapes=[
                pltpu.VMEM((UNIT, dim), BF16),
                pltpu.VMEM((UNIT, width // 2), F32),
                pltpu.VMEM((UNIT * n_heads, head), F32),
                pltpu.VMEM((3, UNIT, n_heads, head), BF16),
                pltpu.VMEM((SLOTS, 3, SPAN, n_heads, head), BF16),
                dma((2, 4)), dma((SLOTS, 3)), dma((SLOTS, 3)), dma((3, 4)),
            ],
            compiler_params=pltpu.CompilerParams(vmem_limit_bytes=room),
            name="finish",
        )(pltpu.with_memory_space_constraint(w2, pltpu.VMEM), gathered, q, k, v)

    row_spec = P(("dp", "tp"), None)
    head_spec = P(None, "tp", None)
    out_spec = P("dp", "tp", None)
    return jax.shard_map(local_step, mesh=mesh, in_specs=(row_spec, P(None), head_spec, head_spec, head_spec), out_specs=(out_spec, out_spec, out_spec), check_vma=False)
```

```python
import functools

import jax
import jax.numpy as jnp
from jax import lax
from jax.experimental import pallas as pl
from jax.experimental.pallas import tpu as pltpu
from jax.sharding import PartitionSpec as P

F32, BF16 = jnp.float32, jnp.bfloat16
MESH_ID = pl.DeviceIdType.MESH

UNIT = 256
PIECE = 64
KC = 2048
EARLY = 2
SLOTS = 10
LAG = 4
SPAN = 128
FIRST_READS = 3
SUB = 32
WB = 256


def fused_kernel(n, x_hbm, gain, wq, wk, wv, q_out, k_out, v_out, gathered, w2, partial,
                 acc, xt, st, ost, wst, xin,
                 in_sem, wb_sem, w_sem, load_sem, out_sem, partial_sem,
                 own_send, own_recv, ici_send, ici_recv, d2d_send, d2d_recv):
    rows, dim = x_hbm.shape
    half = rows // 2
    n_heads, head = wq.shape[1], wq.shape[2]
    width = n_heads * head
    chips = n // 2
    nk = dim // KC
    per_half = half // PIECE
    stage_len = per_half * nk
    n_chunks = 3 * stage_len
    own_units = rows // UNIT
    n_units = n * rows // UNIT - 1
    local_units = 2 * own_units
    n_steps = n_units * nk + EARLY
    weights, outs = (wq, wk, wv), (q_out, k_out, v_out)

    me = lax.axis_index("tp")
    chip, lane = me // 2, me % 2
    sib_lane = 1 - lane
    sibling = chip * 2 + sib_lane
    ahead = (chip + 1) % chips
    behind = (chip + chips - 1) % chips
    dest = (ahead * 2 + lane, behind * 2 + lane)

    barrier = pltpu.get_barrier_semaphore()
    for peer in (dest[0], dest[1], sibling):
        pl.semaphore_signal(barrier, inc=1, device_id={"tp": peer}, device_id_type=MESH_ID)

    def src_row(direction, of_lane, stage, piece):
        dist = 1 + stage // 2
        if direction == 0:
            src, part = (chip + chips - dist) % chips, stage % 2
        else:
            src, part = (chip + dist) % chips, 1 - stage % 2
        return pl.multiple_of((src * 2 + of_lane) * rows + part * half + piece * PIECE, PIECE)

    def own_row(direction, stage, piece):
        part = stage % 2 if direction == 0 else 1 - stage % 2
        return pl.multiple_of(me * rows + part * half + piece * PIECE, PIECE)

    def block(row, kc):
        return gathered.at[pl.ds(row, PIECE), pl.ds(pl.multiple_of(kc * KC, KC), KC)]

    def ici_copy(direction, row, kc, m):
        return pltpu.make_async_remote_copy(
            src_ref=block(row, kc), dst_ref=block(row, kc),
            send_sem=ici_send.at[direction, m], recv_sem=ici_recv.at[direction, m],
            device_id={"tp": dest[direction]}, device_id_type=MESH_ID)

    def d2d_copy(direction, row, kc, m):
        return pltpu.make_async_remote_copy(
            src_ref=block(row, kc), dst_ref=block(row, kc),
            send_sem=d2d_send.at[direction, m], recv_sem=d2d_recv.at[direction, m],
            device_id={"tp": sibling}, device_id_type=MESH_ID)

    def own_copy(owner, idx):
        part, piece = idx % 2, idx // 2
        ref = gathered.at[pl.ds(pl.multiple_of(owner * rows + part * half + piece * PIECE, PIECE), PIECE)]
        return pltpu.make_async_remote_copy(
            src_ref=ref, dst_ref=ref, send_sem=own_send.at[idx], recv_sem=own_recv.at[idx],
            device_id={"tp": sibling}, device_id_type=MESH_ID)

    n_wb = dim // WB

    def w_copy(p, kb, slot):
        buf = (ost, wst)[slot]
        return pltpu.make_async_copy(weights[p].at[pl.ds(pl.multiple_of(kb * WB, WB), WB)], buf.at[p], w_sem.at[slot, p])

    n_pieces = rows // PIECE

    def sub_row(idx, t):
        return pl.multiple_of((idx % 2) * half + (idx // 2) * PIECE + t * SUB, SUB)

    def x_copy(idx, t):
        slot = (idx % 2) * 2 + t
        return pltpu.make_async_copy(x_hbm.at[pl.ds(sub_row(idx, t), SUB)], xin.at[slot], in_sem.at[slot])

    def n_copies(idx, t):
        row = pl.multiple_of(me * rows + sub_row(idx, t), SUB)
        return [pltpu.make_async_copy(
            xt.at[idx % 2, pl.ds((t * nk + kc) * SUB, SUB)],
            gathered.at[pl.ds(row, SUB), pl.ds(kc * KC, KC)], wb_sem.at[(idx % 2) * 2 + t, kc]) for kc in range(nk)]

    for idx in range(2):
        for t in range(2):
            x_copy(idx, t).start()
    for slot in range(2):
        for p in range(3):
            w_copy(p, slot, slot).start()

    cw = min(1024, KC)

    def normalize(idx, t):
        slot = (idx % 2) * 2 + t
        for r in range(0, SUB, 16):
            sq = jnp.zeros((16, cw), F32)
            for c in range(0, dim, cw):
                xv = xin[slot, r:r + 16, c:c + cw].astype(F32)
                sq = sq + xv * xv
            scale = lax.rsqrt(jnp.sum(sq, axis=-1, keepdims=True) * (1.0 / dim) + 1e-6)
            for c in range(0, dim, cw):
                xv = xin[slot, r:r + 16, c:c + cw].astype(F32)
                first = (t * nk + c // KC) * SUB + r
                xt[idx % 2, first:first + 16, c % KC:c % KC + cw] = (xv * scale * gain[:, c:c + cw]).astype(BF16)

    def send_piece(idx):
        piece = idx // 2
        for direction in range(2):
            @pl.when(idx % 2 == direction)
            def _():
                for kc in range(nk):
                    ici_copy(direction, own_row(direction, 0, piece), kc, piece * nk + kc).start()
        own_copy(me, idx).start()

    def norm_half(idx, t):
        x_copy(idx, t).wait()
        normalize(idx, t)

        @pl.when(idx + 2 < n_pieces)
        def _():
            x_copy(idx + 2, t).start()
        for c in n_copies(idx, t):
            c.start()

    def norm_step(idx, _):
        for t in range(2):
            @pl.when(idx < n_pieces)
            def _():
                norm_half(idx, t)

            if t == 0:
                for u in range(2):
                    for c in n_copies(idx - 1, u):
                        c.wait()
                send_piece(idx - 1)
        return 0

    for t in range(2):
        norm_half(0, t)
    pl.semaphore_wait(barrier, 3)
    lax.fori_loop(1, n_pieces + 1, norm_step, 0)

    def unit_rows(t, emit):
        @pl.when(t < own_units)
        def _():
            emit([pl.multiple_of(me * rows + t * UNIT + i * PIECE, PIECE) for i in range(4)])

        @pl.when(jnp.logical_and(t >= own_units, t < local_units))
        def _():
            emit([pl.multiple_of(sibling * rows + (t - own_units) * UNIT + i * PIECE, PIECE) for i in range(4)])

        @pl.when(t >= local_units)
        def _():
            u = t - local_units
            stage, piece = u // per_half, u % per_half
            emit([src_row(d, w, stage, piece) for w in (lane, sib_lane) for d in range(2)])

    def load(s, start):
        t, kc, slot = s // nk, s % nk, s % 2
        if start:
            @pl.when(jnp.logical_and(jnp.logical_and(t >= own_units, t < local_units), kc == 0))
            def _():
                for piece in range(per_half):
                    own_copy(sibling, piece * 2 + (t - own_units)).wait_recv()

            @pl.when(t >= local_units)
            def _():
                u = t - local_units
                for d in range(2):
                    d2d_copy(d, src_row(d, sib_lane, u // per_half, u % per_half), kc, u * nk + kc).wait_recv()

            def emit(row_list):
                for i, row in enumerate(row_list):
                    pltpu.make_async_copy(block(row, kc), xt.at[slot, pl.ds(i * PIECE, PIECE)], load_sem.at[slot, i]).start()
            unit_rows(t, emit)
        else:
            for i in range(4):
                pltpu.make_async_copy(block(0, 0), xt.at[slot, pl.ds(i * PIECE, PIECE)], load_sem.at[slot, i]).wait()

    def handle(m, _):
        u, kc = m // nk, m % nk
        stage, piece = u // per_half, u % per_half
        for d in range(2):
            row = src_row(d, lane, stage, piece)
            ici_copy(d, row, kc, m).wait_recv()
            d2d_copy(d, row, kc, m).start()

            @pl.when(stage == 0)
            def _():
                ici_copy(d, own_row(d, 1, piece), kc, m + stage_len).start()

            @pl.when(stage == 1)
            def _():
                ici_copy(d, src_row(d, lane, 0, piece), kc, m + stage_len).start()
        return 0

    def handled(s):
        return jnp.minimum(n_chunks - nk + EARLY, jnp.maximum(s - (local_units * nk - 2), 4 + (2 * s) // 3))

    load(0, True)

    def relayout(i, _):
        for slot in range(2):
            kb = 2 * i + slot
            buf = (ost, wst)[slot]
            for p in range(3):
                w_copy(p, kb, slot).wait()
                tmp = st.at[p % 2]
                tmp[...] = buf[p].astype(F32).reshape(WB * n_heads, head)
                for h in range(n_heads):
                    w2[pl.ds(pl.multiple_of(kb * WB, WB), WB), p * width + h * head:p * width + (h + 1) * head] = (
                        tmp[pl.ds(h, WB, stride=n_heads), :].astype(BF16))

                @pl.when(kb + 2 < n_wb)
                def _():
                    w_copy(p, kb + 2, slot).start()
        return 0

    lax.fori_loop(0, n_wb // 2, relayout, 0)

    def before(s):
        lax.fori_loop(jnp.where(s == 0, 0, handled(s - 1)), handled(s), handle, 0)

        @pl.when(s + 1 < n_steps)
        def _():
            load(s + 1, True)
        load(s, False)

    def product(s, kc, p):
        depth = pl.ds(pl.multiple_of(kc * KC, KC), KC)
        return jnp.dot(xt[s % 2], w2[depth, p * width:(p + 1) * width], preferred_element_type=F32)

    def store(t, wait):
        if wait:
            for p in range(3):
                for i in range(4):
                    pltpu.make_async_copy(ost.at[p, pl.ds(i * PIECE, PIECE)], outs[p].at[pl.ds(0, PIECE)], out_sem.at[p, i]).wait()
        else:
            def emit(row_list):
                for p in range(3):
                    for i, row in enumerate(row_list):
                        pltpu.make_async_copy(ost.at[p, pl.ds(i * PIECE, PIECE)], outs[p].at[pl.ds(row, PIECE)], out_sem.at[p, i]).start()
            unit_rows(t, emit)

    def partial_step(t, kc, _):
        s = t * nk + kc
        before(s)
        for p in range(3):
            cols = slice(p * width, (p + 1) * width)
            acc[:, cols] = jnp.where(kc == 0, 0.0, acc[:, cols]) + product(s, kc, p)
        return 0

    def unit(t, _):
        lax.fori_loop(0, nk - 1, functools.partial(partial_step, t), 0)
        s = t * nk + nk - 1
        before(s)

        @pl.when(t > 0)
        def _():
            store(t - 1, True)
        for p in range(3):
            total = acc[:, p * width:(p + 1) * width] + product(s, nk - 1, p)
            tmp = st.at[p % 2]
            for h in range(n_heads):
                tmp[pl.ds(h, UNIT, stride=n_heads), :] = total[:, h * head:(h + 1) * head]
            ost[p] = tmp[...].reshape(UNIT, n_heads, head).astype(BF16)
        store(t, False)
        return 0

    lax.fori_loop(0, n_units, unit, 0)
    store(n_units - 1, True)

    lax.fori_loop(0, EARLY, functools.partial(partial_step, n_units), 0)
    keep = pltpu.make_async_copy(acc, partial, partial_sem)
    keep.start()

    def drain(m, _):
        for d in range(2):
            ici_copy(d, 0, 0, m).wait_send()
            d2d_copy(d, 0, 0, m).wait_send()
        return 0

    def drain_own(idx, _):
        own_copy(me, idx).wait_send()
        return 0

    lax.fori_loop(0, n_pieces, drain_own, 0)
    lax.fori_loop(0, n_chunks - nk, drain, 0)

    lax.fori_loop(n_chunks - nk + EARLY, n_chunks, handle, 0)
    lax.fori_loop(n_chunks - nk, n_chunks, drain, 0)
    keep.wait()
    for kc in range(EARLY, nk):
        for d in range(2):
            d2d_copy(d, src_row(d, sib_lane, 2, per_half - 1), kc, n_chunks - nk + kc).wait_recv()


def finish_kernel(n, w2, gathered, partial, q_in, k_in, v_in, q_out, k_out, v_out,
                  xt, acc, st, ost, buf, load_sem, acc_sem, read_sem, write_sem, out_sem):
    ins, outs = (q_in, k_in, v_in), (q_out, k_out, v_out)
    total_rows, dim = gathered.shape
    rows = total_rows // n
    half = rows // 2
    n_heads, head = q_in.shape[1], q_in.shape[2]
    width = n_heads * head
    chips = n // 2
    chip_rows = 2 * rows
    slots, span = buf.shape[0], buf.shape[2]
    first = EARLY * KC
    deep = dim - first

    me = lax.axis_index("tp")
    lane = me % 2
    far = (me // 2 + chips // 2) % chips
    unit_rows = [pl.multiple_of((far * 2 + w) * rows + end - PIECE, PIECE) for w in (lane, 1 - lane) for end in (half, rows)]
    moves = []
    for other in range(1, chips):
        base = ((far + other) % chips) * chip_rows
        moves += [(pl.multiple_of(base + r, PIECE), span) for r in range(0, chip_rows, span)]
    for part in range(0, chip_rows, half):
        for r in range(0, half - PIECE, span):
            moves.append((pl.multiple_of(far * chip_rows + part + r, PIECE), min(span, half - PIECE - r)))

    def read(j):
        row, size = moves[j]
        return [pltpu.make_async_copy(ins[p].at[pl.ds(row, size)], buf.at[j % slots, p, pl.ds(0, size)], read_sem.at[j % slots, p]) for p in range(3)]

    def write(j):
        row, size = moves[j]
        return [pltpu.make_async_copy(buf.at[j % slots, p, pl.ds(0, size)], outs[p].at[pl.ds(row, size)], write_sem.at[j % slots, p]) for p in range(3)]

    def start(copies):
        for c in copies:
            c.start()

    def wait(copies):
        for c in copies:
            c.wait()

    n_cols = width // 2
    n_dots = 3 * width // n_cols
    heads = n_cols // head
    loads = [pltpu.make_async_copy(
        gathered.at[pl.ds(row, PIECE), pl.ds(first, deep)], xt.at[pl.ds(i * PIECE, PIECE)], load_sem.at[i])
        for i, row in enumerate(unit_rows)]
    sums = [pltpu.make_async_copy(partial.at[:, pl.ds(i * n_cols, n_cols)], acc.at[:, pl.ds(i * n_cols, n_cols)], acc_sem.at[i])
            for i in range(n_dots)]

    def result(p):
        return [pltpu.make_async_copy(ost.at[p, pl.ds(i * PIECE, PIECE)], outs[p].at[pl.ds(row, PIECE)], out_sem.at[p, i])
                for i, row in enumerate(unit_rows)]

    start(loads)
    start(sums[:1])
    for j in range(FIRST_READS):
        start(read(j))
    start(sums[1:])
    for j in range(FIRST_READS, slots):
        start(read(j))

    count = {"read": slots, "written": 0, "freed": 0}

    def advance():
        j = count["written"]
        wait(read(j))
        start(write(j))
        count["written"] += 1
        if count["written"] - count["freed"] > LAG:
            wait(write(count["freed"]))
            count["freed"] += 1
            if count["read"] < len(moves):
                start(read(count["read"]))
                count["read"] += 1

    wait(loads)
    for i_dot in range(n_dots):
        p, cols = i_dot // 2, slice(i_dot * n_cols, (i_dot + 1) * n_cols)
        wait(sums[i_dot:i_dot + 1])
        part = acc[:, cols] + jnp.dot(xt[...], w2[first:, cols], preferred_element_type=F32)
        for i in range(heads):
            st[pl.ds((i_dot % 2) * heads + i, UNIT, stride=n_heads), :] = part[:, i * head:(i + 1) * head]
        if i_dot % 2 == 1:
            ost[p] = st[...].reshape(UNIT, n_heads, head).astype(BF16)
            start(result(p))
        for _ in range(3):
            advance()
    while count["written"] < len(moves):
        advance()
    for j in range(count["freed"], len(moves)):
        wait(write(j))
    for p in range(3):
        wait(result(p))


def solution(mesh):
    n = mesh.shape["tp"]

    def local_step(hidden_blk, norm_gain, wq_local, wk_local, wv_local):
        rows, dim = hidden_blk.shape
        n_heads, head = wq_local.shape[1:]
        width = n_heads * head
        chunks = 3 * (rows // 2 // PIECE) * (dim // KC)
        out = jax.ShapeDtypeStruct((n * rows, n_heads, head), BF16)
        dma = pltpu.SemaphoreType.DMA
        hbm = pl.BlockSpec(memory_space=pl.ANY)
        vmem = pl.BlockSpec(memory_space=pltpu.VMEM)
        room = 67043328 - 2 * dim * 3 * width
        q, k, v, gathered, w2, partial = pl.pallas_call(
            functools.partial(fused_kernel, n),
            out_shape=(out, out, out, jax.ShapeDtypeStruct((n * rows, dim), BF16), pltpu.VMEM((dim, 3 * width), BF16),
                       jax.ShapeDtypeStruct((UNIT, 3 * width), F32)),
            in_specs=[hbm, vmem, hbm, hbm, hbm],
            out_specs=(hbm, hbm, hbm, hbm, vmem, hbm),
            scratch_shapes=[
                pltpu.VMEM((UNIT, 3 * width), F32),
                pltpu.VMEM((2, UNIT, KC), BF16),
                pltpu.VMEM((2, UNIT * n_heads, head), F32),
                pltpu.VMEM((3, UNIT, n_heads, head), BF16),
                pltpu.VMEM((3, WB, n_heads, head), BF16),
                pltpu.VMEM((4, SUB, dim), BF16),
                dma((4,)), dma((4, dim // KC)), dma((2, 3)), dma((2, 4)), dma((3, 4)), dma,
                dma((rows // PIECE,)), dma((rows // PIECE,)),
                dma((2, chunks)), dma((2, chunks)), dma((2, chunks)), dma((2, chunks)),
            ],
            compiler_params=pltpu.CompilerParams(
                collective_id=0, has_side_effects=True, vmem_limit_bytes=room),
            name="norm_gather_project",
        )(hidden_blk, norm_gain.reshape(1, dim), wq_local, wk_local, wv_local)
        return pl.pallas_call(
            functools.partial(finish_kernel, n),
            out_shape=(out, out, out),
            in_specs=[vmem, hbm, hbm, hbm, hbm, hbm],
            out_specs=(hbm, hbm, hbm),
            scratch_shapes=[
                pltpu.VMEM((UNIT, dim - EARLY * KC), BF16),
                pltpu.VMEM((UNIT, 3 * width), F32),
                pltpu.VMEM((UNIT * n_heads, head), F32),
                pltpu.VMEM((3, UNIT, n_heads, head), BF16),
                pltpu.VMEM((SLOTS, 3, SPAN, n_heads, head), BF16),
                dma((4,)), dma((6,)), dma((SLOTS, 3)), dma((SLOTS, 3)), dma((3, 4)),
            ],
            compiler_params=pltpu.CompilerParams(vmem_limit_bytes=room),
            name="finish",
        )(pltpu.with_memory_space_constraint(w2, pltpu.VMEM), gathered, partial, q, k, v)

    row_spec = P(("dp", "tp"), None)
    head_spec = P(None, "tp", None)
    out_spec = P("dp", "tp", None)
    return jax.shard_map(local_step, mesh=mesh, in_specs=(row_spec, P(None), head_spec, head_spec, head_spec), out_specs=(out_spec, out_spec, out_spec), check_vma=False)
```
